32 devices in a mesh: dp: 8 (over z, core), tensor: 4 (over y, x).
Axes of the slice: x: 2, y: 2, z: 4, core: 2. Of those that a mesh axis runs over, the one named last changes fastest.
Arguments:
- saved_queries: bfloat16 [4096, 8192], P('dp', 'tensor'), may hold values from -200 to 200
- saved_keys: bfloat16 [4096, 1024], P('dp', 'tensor'), may hold values from -200 to 200
- saved_values: bfloat16 [4096, 1024], P('dp', 'tensor'), may hold values from -6 to 6
- out_grad: bfloat16 [4096, 8192], P(('dp', 'tensor')), may hold values from -0.59765625 to 0.59765625
- act_exponent: int32 [1], replicated, may hold values from -6 to 3
- grad_exponent: int32 [1], replicated, may hold values from -4 to 1
Outputs:
- grad_weight: float32 [8192, 8192], P('dp', 'tensor')
The draws below stay inside these ranges and needn't reach their ends.
All inputs are finite; a program needn't handle non-finite values.
Results may differ from the reference program's by a relative error of at most 0.012.
Values may be sent and summed in bfloat16 or wider, within the bound.
A program may use at most 128 MiB of HBM per device.

```python
import jax
import jax.numpy as jnp
from jax import lax

D = 8192
HEADS = 64
KV_HEADS = 8
HEAD_DIM = 128
SEQ = 512
TOKENS = 4096
N_DP = 8


def query_keys(key):
    base = jax.random.fold_in(key, 11)
    first, second = jax.random.split(base)
    queries = jnp.clip(jax.random.normal(first, (TOKENS, HEADS * HEAD_DIM), jnp.float32), -5.0, 5.0)
    keys_all = jnp.clip(jax.random.normal(second, (TOKENS, KV_HEADS * HEAD_DIM), jnp.float32), -5.0, 5.0)
    return (queries, keys_all)


def draw_saved_queries(key, part):
    return query_keys(key)[0].astype(jnp.bfloat16)


def draw_saved_keys(key, part):
    return query_keys(key)[1].astype(jnp.bfloat16)


def raised(entries, stream_key, source, target, parts, factor):
    def block_of(axis_at):
        return (jnp.arange(entries.shape[axis_at]) // (entries.shape[axis_at] // parts)).reshape((-1,) + (1,) * (entries.ndim - 1 - axis_at))

    near = jax.random.permutation(stream_key, parts)[block_of(target)]
    second = (block_of(target) + parts // 2) % parts
    return jnp.where((block_of(source) == near) | (block_of(source) == second), factor * entries, entries)


def steps_of(rng, extent, cuts, low, largest):
    factor_of = 1.0
    for dim, blocks in cuts:
        steps = jax.random.uniform(jax.random.fold_in(jax.random.fold_in(rng, 6), dim), (blocks,), jnp.float32, low / len(cuts), largest / len(cuts))
        factor_of = factor_of * jnp.repeat(jnp.exp(steps), extent[dim] // blocks).reshape((-1,) + (1,) * (len(extent) - 1 - dim))
    return factor_of


def centred(key, shape, deviation, reach, cuts=(), kind=jnp.bfloat16):
    array = jax.random.normal(key, shape, jnp.float32) * deviation
    if len(cuts) > 0:
        array = steps_of(key, shape, cuts, -0.22, 0.18) * array
    return jnp.clip(array, min=-reach, max=reach).astype(kind)


def heavy_noise(rng, shape, width, limit, shards, heavy, kind=jnp.bfloat16):
    drawn = width * jax.random.normal(rng, shape, jnp.float32)
    if shards:
        drawn = drawn * steps_of(rng, shape, shards, -0.22, 0.18)
    return jnp.clip(raised(drawn, jax.random.fold_in(rng, 3), *heavy), -limit, limit).astype(kind)


def setup_inputs(seed: int = 0) -> dict:
    splits = jax.random.split(jax.random.key(seed), 7)
    return {
        "saved_queries": draw_saved_queries(jax.random.fold_in(splits[6], 71), 0),
        "saved_keys": draw_saved_keys(jax.random.fold_in(splits[6], 71), 0),
        "saved_values": centred(splits[2], (TOKENS, KV_HEADS * HEAD_DIM), 1.0, 6.0, ((0, 8), (1, 4))),
        "out_grad": heavy_noise(splits[3], (TOKENS, D), 0.1, 0.59765625, ((0, 32),), (0, 1, 32, 2.75)),
        "act_exponent": jax.random.randint(splits[4], (1,), -6, 4).astype(jnp.int32),
        "grad_exponent": jax.random.randint(splits[5], (1,), -4, 2).astype(jnp.int32),
    }


SATURATION = 448.0

def quantize(values_in, exponent):
    factor = SATURATION * jnp.exp2(-exponent[0].astype(jnp.float32))
    return jnp.clip(values_in * factor, -SATURATION, SATURATION).astype(jnp.bfloat16)

def attend(query_rows, key_rows, value_rows):
    scores = jnp.dot(query_rows, key_rows.T, preferred_element_type=jnp.float32) * HEAD_DIM ** (-0.5)
    positions = jnp.arange(query_rows.shape[0], dtype=jnp.int32)
    causal = positions[None, :] <= positions[:, None]
    scores = jnp.where(causal, scores, jnp.float32(-1e+30))
    row_max = lax.optimization_barrier(jnp.max(scores, axis=1, keepdims=True))
    weights = jnp.exp(scores - row_max)
    probabilities = (weights / lax.optimization_barrier(jnp.sum(weights, axis=1, keepdims=True))).astype(jnp.bfloat16)
    return jnp.dot(probabilities, value_rows, preferred_element_type=jnp.float32)

def reference(saved_queries, saved_keys, saved_values, out_grad, act_exponent, grad_exponent):
    per_group = HEADS // KV_HEADS
    dequant = jnp.exp2((act_exponent[0] + grad_exponent[0]).astype(jnp.float32)) / (SATURATION * SATURATION)

    def sequence_grad(running, seq_index):
        offset = (seq_index * SEQ).astype(jnp.int32)
        seq_queries = lax.dynamic_slice_in_dim(saved_queries, offset, SEQ, 0)
        seq_keys = lax.dynamic_slice_in_dim(saved_keys, offset, SEQ, 0)
        seq_values = lax.dynamic_slice_in_dim(saved_values, offset, SEQ, 0)
        seq_grad = lax.dynamic_slice_in_dim(out_grad, offset, SEQ, 0)

        def one_head(head_index):
            query_rows = lax.dynamic_slice_in_dim(seq_queries, (head_index * HEAD_DIM).astype(jnp.int32), HEAD_DIM, 1)
            kv_start = (head_index // per_group * HEAD_DIM).astype(jnp.int32)
            key_rows = lax.dynamic_slice_in_dim(seq_keys, kv_start, HEAD_DIM, 1)
            value_rows = lax.dynamic_slice_in_dim(seq_values, kv_start, HEAD_DIM, 1)
            return attend(query_rows, key_rows, value_rows)
        attended = lax.map(one_head, jnp.arange(HEADS, dtype=jnp.int32))
        attended = jnp.transpose(attended, (1, 0, 2)).reshape(SEQ, HEADS * HEAD_DIM)
        act_scaled = quantize(attended, act_exponent)
        grad_scaled = quantize(seq_grad.astype(jnp.float32), grad_exponent)
        seq_partial = lax.dot_general(grad_scaled, act_scaled, (((0,), (0,)), ((), ())), preferred_element_type=jnp.float32)
        seq_partial = (seq_partial * dequant).astype(jnp.bfloat16)
        return (running + seq_partial.astype(jnp.float32), None)
    zero_sum = jnp.zeros((D, HEADS * HEAD_DIM), jnp.float32)
    grad_weight, unused = lax.scan(sequence_grad, zero_sum, jnp.arange(N_DP, dtype=jnp.int32))
    return grad_weight
```

```python
import functools

import jax
import jax.numpy as jnp
from jax import lax
from jax.experimental import pallas as pl
from jax.experimental.pallas import tpu as pltpu
from jax.sharding import PartitionSpec as P

HEAD_DIM = 128
SATURATION = 448.0
CHUNKS = 4


def quantize(values_in, exponent):
    factor = SATURATION * jnp.exp2(-exponent[0].astype(jnp.float32))
    return jnp.clip(values_in * factor, -SATURATION, SATURATION).astype(jnp.bfloat16)


def attend_group(queries, key_rows, value_rows):
    seq_len = queries.shape[0]
    heads = queries.shape[1] // HEAD_DIM
    stacked = queries.reshape(seq_len, heads, HEAD_DIM)
    scores = jnp.einsum(
        "thd,ud->htu", stacked, key_rows, preferred_element_type=jnp.float32
    ) * HEAD_DIM ** (-0.5)
    positions = jnp.arange(seq_len, dtype=jnp.int32)
    causal = positions[None, :] <= positions[:, None]
    scores = jnp.where(causal[None], scores, jnp.float32(-1e30))
    row_max = jnp.max(scores, axis=2, keepdims=True)
    weights = jnp.exp(scores - row_max)
    probabilities = (weights / jnp.sum(weights, axis=2, keepdims=True)).astype(jnp.bfloat16)
    out = jnp.einsum(
        "htu,ud->thd", probabilities, value_rows, preferred_element_type=jnp.float32
    )
    return out.reshape(seq_len, heads * HEAD_DIM)


def gather_kernel(
    n_dp, n_t, act_ref, grad_ref, act_out, grad_out,
    a_send, a_recv, b_send, b_recv, c_send, c_recv, p_send, p_recv, own_sem,
):
    dp = lax.axis_index("dp")
    t = lax.axis_index("tensor")
    core = dp % 2
    z = dp // 2
    n_z = n_dp // 2
    partner = dp + 1 - 2 * core
    rows = act_ref.shape[0] // CHUNKS

    barrier = pltpu.get_barrier_semaphore()
    for k in range(1, n_dp):
        pl.semaphore_signal(
            barrier, inc=1, device_id={"dp": (dp + k) % n_dp, "tensor": t},
            device_id_type=pl.DeviceIdType.MESH,
        )
    for j in range(1, n_t):
        pl.semaphore_signal(
            barrier, inc=1, device_id={"dp": dp, "tensor": (t + j) % n_t},
            device_id_type=pl.DeviceIdType.MESH,
        )
    pl.semaphore_wait(barrier, n_dp + n_t - 2)

    def remote(src, dst, send, recv, to_dp, to_t):
        return pltpu.make_async_remote_copy(
            src_ref=src, dst_ref=dst, send_sem=send, recv_sem=recv,
            device_id={"dp": to_dp, "tensor": to_t}, device_id_type=pl.DeviceIdType.MESH,
        )

    def stage_a(k):
        to = (dp + k) % n_dp
        return remote(
            grad_ref.at[to], grad_out.at[dp, t], a_send.at[k], a_recv.at[k], to, t
        )

    def stage_b(k, j):
        owner = (dp + n_dp - k) % n_dp
        src = grad_ref.at[dp] if k == 0 else grad_out.at[owner, t]
        return remote(
            src, grad_out.at[owner, t], b_send.at[k, j], b_recv.at[k, j], dp, (t + j) % n_t
        )

    def part(block, q):
        return act_out.at[block, pl.ds(q * rows, rows)]

    def chain(side, i, q):
        step = 1 - 2 * side
        block = (z - i * step) * 2 + core
        src = act_ref.at[pl.ds(q * rows, rows)] if i == 0 else part(block, q)
        return remote(
            src, part(block, q), c_send.at[side, i, q], c_recv.at[side, i, q],
            dp + 2 * step, t,
        )

    def can_send(side, i):
        if side == 0:
            return (z - i >= 0) & (z + 1 < n_z)
        return (z + i < n_z) & (z - 1 >= 0)

    def can_take(side, i):
        return z - 1 - i >= 0 if side == 0 else z + 1 + i < n_z

    def share(side, i, q):
        step = 1 - 2 * side
        block = (z - (i + 1) * step) * 2 + core
        return remote(
            part(block, q), part(block, q), p_send.at[side, i, q], p_recv.at[side, i, q],
            partner, t,
        )

    def share_own(q):
        return remote(
            act_ref.at[pl.ds(q * rows, rows)], part(dp, q),
            p_send.at[0, n_z - 1, q], p_recv.at[0, n_z - 1, q], partner, t,
        )

    for k in range(1, n_dp):
        stage_a(k).start()
    for q in range(CHUNKS):
        for side in range(2):
            @pl.when(can_send(side, 0))
            def _():
                chain(side, 0, q).start()
    for j in range(1, n_t):
        stage_b(0, j).start()
    for q in range(CHUNKS):
        share_own(q).start()
    own_act = pltpu.make_async_copy(act_ref, act_out.at[dp], own_sem.at[0])
    own_grad = pltpu.make_async_copy(grad_ref.at[dp], grad_out.at[dp, t], own_sem.at[1])
    own_act.start()
    own_grad.start()
    for k in range(1, n_dp):
        stage_a(k).wait_recv()
        for j in range(1, n_t):
            stage_b(k, j).start()
    for i in range(n_z - 1):
        for q in range(CHUNKS):
            for side in range(2):
                @pl.when(can_take(side, i))
                def _():
                    chain(side, i, q).wait_recv()
                    if i + 1 < n_z - 1:
                        @pl.when(can_send(side, i + 1))
                        def _():
                            chain(side, i + 1, q).start()
                    share(side, i, q).start()
    own_act.wait()
    own_grad.wait()
    for q in range(CHUNKS):
        share_own(q).wait()
    for k in range(1, n_dp):
        stage_a(k).wait_send()
    for k in range(n_dp):
        for j in range(1, n_t):
            stage_b(k, j).wait()
    for i in range(n_z - 1):
        for q in range(CHUNKS):
            for side in range(2):
                @pl.when(can_send(side, i))
                def _():
                    chain(side, i, q).wait_send()

                @pl.when(can_take(side, i))
                def _():
                    share(side, i, q).wait()


def gather_all(act, grad_blocks, n_t):
    n_dp, rows, cols = grad_blocks.shape
    n_z = n_dp // 2
    dma = pltpu.SemaphoreType.DMA
    return pl.pallas_call(
        functools.partial(gather_kernel, n_dp, n_t),
        out_shape=(
            jax.ShapeDtypeStruct((n_dp,) + act.shape, act.dtype),
            jax.ShapeDtypeStruct((n_dp, n_t, rows, cols), act.dtype),
        ),
        in_specs=[pl.BlockSpec(memory_space=pltpu.VMEM)] * 2,
        out_specs=(pl.BlockSpec(memory_space=pl.ANY),) * 2,
        scratch_shapes=[
            dma((n_dp,)), dma((n_dp,)),
            dma((n_dp, n_t)), dma((n_dp, n_t)),
            dma((2, n_z, CHUNKS)), dma((2, n_z, CHUNKS)),
            dma((2, n_z, CHUNKS)), dma((2, n_z, CHUNKS)),
            dma((2,)),
        ],
        compiler_params=pltpu.CompilerParams(
            collective_id=0, has_side_effects=True, vmem_limit_bytes=60 * 1024 * 1024
        ),
    )(act, grad_blocks)


def on_device(n_dp, n_t, saved_queries, saved_keys, saved_values, out_grad, act_exponent, grad_exponent):
    groups = saved_keys.shape[1] // HEAD_DIM
    width = saved_queries.shape[1] // groups
    dequant = jnp.exp2((act_exponent[0] + grad_exponent[0]).astype(jnp.float32)) / (
        SATURATION * SATURATION
    )
    rows, d_model = out_grad.shape
    cols = d_model // n_dp
    grad_scaled = quantize(out_grad.astype(jnp.float32), grad_exponent)
    grad_blocks = grad_scaled.reshape(rows, n_dp, cols).transpose(1, 0, 2)
    acts = []
    for g in range(groups):
        k = saved_keys[:, g * HEAD_DIM:(g + 1) * HEAD_DIM]
        v = saved_values[:, g * HEAD_DIM:(g + 1) * HEAD_DIM]
        q = saved_queries[:, g * width:(g + 1) * width]
        acts.append(quantize(attend_group(q, k, v), act_exponent))
    act = jnp.concatenate(acts, axis=1)
    act_all, grad_all = gather_all(act, grad_blocks, n_t)
    act_rows = act_all.reshape(-1, act.shape[1])
    grad_rows = grad_all.reshape(-1, cols)
    return lax.dot_general(
        grad_rows, act_rows, (((0,), (0,)), ((), ())), preferred_element_type=jnp.float32
    ) * dequant


def solution(mesh):
    in_specs = (
        P("dp", "tensor"),
        P("dp", "tensor"),
        P("dp", "tensor"),
        P(("dp", "tensor"), None),
        P(),
        P(),
    )
    return jax.shard_map(
        functools.partial(on_device, mesh.shape["dp"], mesh.shape["tensor"]),
        mesh=mesh,
        in_specs=in_specs, out_specs=P("dp", "tensor"), check_vma=False
    )
```

```python
import functools

import jax
import jax.numpy as jnp
from jax import lax
from jax.experimental import pallas as pl
from jax.experimental.pallas import tpu as pltpu
from jax.sharding import PartitionSpec as P

HEAD_DIM = 128
SATURATION = 448.0
CHUNKS = 2


def quantize(values_in, exponent):
    factor = SATURATION * jnp.exp2(-exponent[0].astype(jnp.float32))
    return jnp.clip(values_in * factor, -SATURATION, SATURATION).astype(jnp.bfloat16)


def attend_group(queries, key_rows, value_rows):
    seq_len = queries.shape[0]
    heads = queries.shape[1] // HEAD_DIM
    stacked = queries.reshape(seq_len, heads, HEAD_DIM)
    scores = jnp.einsum(
        "thd,ud->htu", stacked, key_rows, preferred_element_type=jnp.float32
    ) * HEAD_DIM ** (-0.5)
    positions = jnp.arange(seq_len, dtype=jnp.int32)
    causal = positions[None, :] <= positions[:, None]
    scores = jnp.where(causal[None], scores, jnp.float32(-1e30))
    row_max = jnp.max(scores, axis=2, keepdims=True)
    weights = jnp.exp(scores - row_max)
    probabilities = (weights / jnp.sum(weights, axis=2, keepdims=True)).astype(jnp.bfloat16)
    out = jnp.einsum(
        "htu,ud->thd", probabilities, value_rows, preferred_element_type=jnp.float32
    )
    return out.reshape(seq_len, heads * HEAD_DIM)


def gather_kernel(
    n_dp, n_t, groups, *refs
):
    act_refs, grad_refs = refs[:groups], refs[groups:groups + n_dp]
    act_out, grad_out = refs[groups + n_dp:groups + n_dp + 2]
    b_send, b_recv, c_send, c_recv, p_send, p_recv, own_sem = refs[groups + n_dp + 2:]
    chunks = CHUNKS * groups
    dp = lax.axis_index("dp")
    t = lax.axis_index("tensor")
    core = dp % 2
    z = dp // 2
    n_z = n_dp // 2
    partner = dp + 1 - 2 * core
    rows = act_refs[0].shape[0] // CHUNKS
    width = act_refs[0].shape[1]

    barrier = pltpu.get_barrier_semaphore()
    for k in range(1, n_dp):
        pl.semaphore_signal(
            barrier, inc=1, device_id={"dp": (dp + k) % n_dp, "tensor": t},
            device_id_type=pl.DeviceIdType.MESH,
        )
    for j in range(1, n_t):
        pl.semaphore_signal(
            barrier, inc=1, device_id={"dp": dp, "tensor": (t + j) % n_t},
            device_id_type=pl.DeviceIdType.MESH,
        )
    pl.semaphore_wait(barrier, n_dp + n_t - 2)

    def remote(src, dst, send, recv, to_dp, to_t):
        return pltpu.make_async_remote_copy(
            src_ref=src, dst_ref=dst, send_sem=send, recv_sem=recv,
            device_id={"dp": to_dp, "tensor": to_t}, device_id_type=pl.DeviceIdType.MESH,
        )

    def stage_b(k, j):
        owner = (dp + n_dp - k) % n_dp
        return remote(
            grad_refs[k], grad_out.at[owner, t], b_send.at[k, j], b_recv.at[k, j], dp, (t + j) % n_t
        )

    def part(block, q):
        return act_out.at[
            block, pl.ds(q % CHUNKS * rows, rows), pl.ds(q // CHUNKS * width, width)
        ]

    def own_part(q):
        return act_refs[q // CHUNKS].at[pl.ds(q % CHUNKS * rows, rows)]

    def chain(side, i, q):
        step = 1 - 2 * side
        block = (z - i * step) * 2 + core
        src = own_part(q) if i == 0 else part(block, q)
        return remote(
            src, part(block, q), c_send.at[side, i, q], c_recv.at[side, i, q],
            dp + 2 * step, t,
        )

    def can_send(side, i):
        if side == 0:
            return (z - i >= 0) & (z + 1 < n_z)
        return (z + i < n_z) & (z - 1 >= 0)

    def can_take(side, i):
        return z - 1 - i >= 0 if side == 0 else z + 1 + i < n_z

    def share(side, i, q):
        step = 1 - 2 * side
        block = (z - (i + 1) * step) * 2 + core
        return remote(
            part(block, q), part(block, q), p_send.at[side, i, q], p_recv.at[side, i, q],
            partner, t,
        )

    def share_own(q):
        return remote(
            own_part(q), part(dp, q),
            p_send.at[0, n_z - 1, q], p_recv.at[0, n_z - 1, q], partner, t,
        )

    for q in range(chunks):
        for side in range(2):
            @pl.when(can_send(side, 0))
            def _():
                chain(side, 0, q).start()
    for k in range(n_dp):
        for j in range(1, n_t):
            stage_b(k, j).start()
    for q in range(chunks):
        share_own(q).start()

    def own_act(q):
        return pltpu.make_async_copy(own_part(q), part(dp, q), own_sem.at[n_dp + q])

    for q in range(chunks):
        own_act(q).start()

    def own_grad(k):
        return pltpu.make_async_copy(
            grad_refs[k], grad_out.at[(dp + n_dp - k) % n_dp, t], own_sem.at[k]
        )

    for k in range(n_dp):
        own_grad(k).start()
    for i in range(n_z - 1):
        for q in range(chunks):
            for side in range(2):
                @pl.when(can_take(side, i))
                def _():
                    chain(side, i, q).wait_recv()
                    if i + 1 < n_z - 1:
                        @pl.when(can_send(side, i + 1))
                        def _():
                            chain(side, i + 1, q).start()
                    share(side, i, q).start()
    for q in range(chunks):
        own_act(q).wait()
    for k in range(n_dp):
        own_grad(k).wait()
    for q in range(chunks):
        share_own(q).wait()
    for k in range(n_dp):
        for j in range(1, n_t):
            stage_b(k, j).wait()
    for i in range(n_z - 1):
        for q in range(chunks):
            for side in range(2):
                @pl.when(can_send(side, i))
                def _():
                    chain(side, i, q).wait_send()

                @pl.when(can_take(side, i))
                def _():
                    share(side, i, q).wait()


def gather_all(acts, grad_blocks, n_t):
    n_dp, groups = len(grad_blocks), len(acts)
    rows, cols = grad_blocks[0].shape
    seq_len, width = acts[0].shape
    n_z, chunks = n_dp // 2, CHUNKS * groups
    dtype = acts[0].dtype
    dma = pltpu.SemaphoreType.DMA
    return pl.pallas_call(
        functools.partial(gather_kernel, n_dp, n_t, groups),
        out_shape=(
            jax.ShapeDtypeStruct((n_dp, seq_len, groups * width), dtype),
            jax.ShapeDtypeStruct((n_dp, n_t, rows, cols), dtype),
        ),
        in_specs=[pl.BlockSpec(memory_space=pltpu.VMEM)] * (groups + n_dp),
        out_specs=(pl.BlockSpec(memory_space=pl.ANY),) * 2,
        scratch_shapes=[
            dma((n_dp, n_t)), dma((n_dp, n_t)),
            dma((2, n_z, chunks)), dma((2, n_z, chunks)),
            dma((2, n_z, chunks)), dma((2, n_z, chunks)),
            dma((n_dp + chunks,)),
        ],
        compiler_params=pltpu.CompilerParams(
            collective_id=0, has_side_effects=True, vmem_limit_bytes=60 * 1024 * 1024
        ),
    )(*acts, *grad_blocks)


def on_device(n_dp, n_t, saved_queries, saved_keys, saved_values, out_grad, act_exponent, grad_exponent):
    groups = saved_keys.shape[1] // HEAD_DIM
    width = saved_queries.shape[1] // groups
    dequant = jnp.exp2((act_exponent[0] + grad_exponent[0]).astype(jnp.float32)) / (
        SATURATION * SATURATION
    )
    rows, d_model = out_grad.shape
    cols = d_model // n_dp
    grad_scaled = quantize(out_grad.astype(jnp.float32), grad_exponent)
    dp = lax.axis_index("dp")
    blocks = []
    for k in range(n_dp):
        to = (dp + k) % n_dp
        block = lax.dynamic_slice_in_dim(grad_scaled, to * cols, cols, 1)
        if k > 0:
            block = lax.ppermute(block, "dp", [(d, (d + k) % n_dp) for d in range(n_dp)])
        blocks.append(block)
    acts = []
    for g in range(groups):
        k = saved_keys[:, g * HEAD_DIM:(g + 1) * HEAD_DIM]
        v = saved_values[:, g * HEAD_DIM:(g + 1) * HEAD_DIM]
        q = saved_queries[:, g * width:(g + 1) * width]
        acts.append(quantize(attend_group(q, k, v), act_exponent))
    act_all, grad_all = gather_all(acts, blocks, n_t)
    act_rows = act_all.reshape(-1, act_all.shape[2])
    grad_rows = grad_all.reshape(-1, cols)
    return lax.dot_general(
        grad_rows, act_rows, (((0,), (0,)), ((), ())), preferred_element_type=jnp.float32
    ) * dequant


def solution(mesh):
    in_specs = (
        P("dp", "tensor"),
        P("dp", "tensor"),
        P("dp", "tensor"),
        P(("dp", "tensor"), None),
        P(),
        P(),
    )
    return jax.shard_map(
        functools.partial(on_device, mesh.shape["dp"], mesh.shape["tensor"]),
        mesh=mesh,
        in_specs=in_specs, out_specs=P("dp", "tensor"), check_vma=False
    )
```
